8 devices in a mesh: proto: 4 (over z, y, x), data: 2 (over core).
Axes of the slice: x: 2, y: 2, z: 1, core: 2. Of those that a mesh axis runs over, the one named last changes fastest.
Arguments:
- emb_one: bfloat16 [4096, 256], P('data')
- emb_two: bfloat16 [4096, 256], P('data')
- protos: bfloat16 [1024, 256], P('proto')
Outputs:
- output 1: float32 [4096, 1024], P('data', 'proto')
- output 2: float32 [4096, 1024], P('data', 'proto')
- output 3: float32 [], replicated
- output 4: float32 [4096, 256], P('data')
- output 5: float32 [4096, 256], P('data')
- output 6: float32 [1024, 256], P('proto')
All inputs are finite; a program needn't handle non-finite values.
Results may differ from the reference program's by a relative error of at most 0.001.
Values are sent between devices in bfloat16 or wider.
A program may use at most 1 GiB of HBM per device.

```python
import jax
import jax.numpy as jnp

ROWS_DEV = 2048
DATA_GROUPS = 2
NUM_PROTOS = 1024
EMBED_DIM = 256
SINKHORN_ITERS = 3
EPSILON = 0.05
TEMP_TAU = 0.1
NOISE_SCALE = 0.8
TOTAL_ROWS = ROWS_DEV * DATA_GROUPS


def unit_rows(matrix):
    return matrix / jnp.sqrt(jnp.sum(matrix * matrix, axis=1, keepdims=True))


def setup_inputs(seed: int = 0) -> dict:
    key = jax.random.key(seed)
    key_protos, key_home, key_one, key_two = jax.random.split(key, 4)
    protos = unit_rows(jax.random.normal(key_protos, (NUM_PROTOS, EMBED_DIM), jnp.float32))
    shard_ids = jnp.arange(TOTAL_ROWS, dtype=jnp.int32) // ROWS_DEV
    home_ids = shard_ids + DATA_GROUPS * jax.random.randint(key_home, (TOTAL_ROWS,), 0, NUM_PROTOS // DATA_GROUPS)
    centers = protos[home_ids]
    noise_one = jax.random.normal(key_one, (TOTAL_ROWS, EMBED_DIM), jnp.float32) * (NOISE_SCALE * EMBED_DIM ** -0.5)
    noise_two = jax.random.normal(key_two, (TOTAL_ROWS, EMBED_DIM), jnp.float32) * (NOISE_SCALE * EMBED_DIM ** -0.5)
    return {'emb_one': unit_rows(centers + noise_one).astype(jnp.bfloat16),
            'emb_two': unit_rows(centers + noise_two).astype(jnp.bfloat16),
            'protos': protos.astype(jnp.bfloat16)}


def sinkhorn_codes(scores):
    transport = jnp.exp(scores / EPSILON)
    for _ in range(SINKHORN_ITERS):
        col_sum = jnp.sum(transport, axis=0)
        transport = transport / (NUM_PROTOS * col_sum)
        row_sum = jnp.sum(transport, axis=1, keepdims=True)
        transport = transport / (TOTAL_ROWS * row_sum)
    return TOTAL_ROWS * transport


def log_probs(scores):
    logits = scores / TEMP_TAU
    return logits - jnp.log(jnp.sum(jnp.exp(logits), axis=1, keepdims=True))


def reference(emb_one, emb_two, protos):
    scores_one = jnp.dot(emb_one, protos.T, preferred_element_type=jnp.float32)
    scores_two = jnp.dot(emb_two, protos.T, preferred_element_type=jnp.float32)
    codes_one = sinkhorn_codes(scores_one)
    codes_two = sinkhorn_codes(scores_two)
    logp_one = log_probs(scores_one)
    logp_two = log_probs(scores_two)
    loss_value = -(jnp.sum(codes_two * logp_one) + jnp.sum(codes_one * logp_two)) / (2 * TOTAL_ROWS)
    grad_scale = 2 * TOTAL_ROWS * TEMP_TAU
    logit_grad_one = ((jnp.exp(logp_one) - codes_two) / grad_scale).astype(jnp.bfloat16)
    logit_grad_two = ((jnp.exp(logp_two) - codes_one) / grad_scale).astype(jnp.bfloat16)
    grad_one = jnp.dot(logit_grad_one, protos, preferred_element_type=jnp.float32)
    grad_two = jnp.dot(logit_grad_two, protos, preferred_element_type=jnp.float32)
    grad_protos = (jnp.dot(logit_grad_one.T, emb_one, preferred_element_type=jnp.float32)
                   + jnp.dot(logit_grad_two.T, emb_two, preferred_element_type=jnp.float32))
    return codes_one, codes_two, loss_value, grad_one, grad_two, grad_protos
```

```python
import functools

import jax
import jax.numpy as jnp
from jax import lax
from jax.experimental import pallas as pl
from jax.experimental.pallas import tpu as pltpu
from jax.sharding import PartitionSpec as P

EPSILON = 0.05
TEMP_TAU = 0.1
LOG2E = 1.4426950408889634
LN2 = 0.6931471805599453
MESH = pl.DeviceIdType.MESH
F32 = jnp.float32
BF16 = jnp.bfloat16


def groups(x):
    return x.reshape(x.shape[0] // 8, 8, x.shape[1])


def kernel(n_rows_total, z1_hbm, z2_hbm, c_hbm,
           q1_out, q2_out, loss_out, g1_out, g2_out, gp_out,
           z_ref, c_ref, e_ref, f_ref, x_ref, h_ref, d_ref, r_ref, s_ref, l_ref,
           csum_ref, csend_ref, crecv_ref, gsend_ref, grecv_ref, lbuf_ref,
           zsem, csem, ag_send, ag_recv, ex_send, ex_recv, gp_send, gp_recv, ls_send, ls_recv):
    rows = z1_hbm.shape[0]
    cols = c_hbm.shape[0]
    allc = 4 * cols
    p = lax.axis_index("proto")
    d = lax.axis_index("data")
    px = p + 1 - 2 * lax.rem(p, 2)
    py = lax.rem(p + 2, 4)
    pd = 3 - p
    sib = 1 - d
    grad_scale = 1.0 / (2.0 * n_rows_total * TEMP_TAU)

    barrier = pltpu.get_barrier_semaphore()
    peers = [(p, sib)] + [(q, e) for q in (px, py, pd) for e in (d, sib)]
    for q, e in peers:
        pl.semaphore_signal(barrier, inc=1, device_id=(q, e), device_id_type=MESH)
    cc = pltpu.make_async_copy(c_hbm, c_ref.at[pl.ds(0, cols)], csem)
    cc.start()
    zc = [pltpu.make_async_copy(z, z_ref.at[v], zsem.at[v]) for v, z in enumerate((z1_hbm, z2_hbm))]
    for k in zc:
        k.start()
    cc.wait()
    pl.semaphore_wait(barrier, 7)
    ag = []
    for i, q in enumerate((px, py, pd)):
        k = pltpu.make_async_remote_copy(
            src_ref=c_ref.at[pl.ds(0, cols)], dst_ref=c_ref.at[pl.ds((i + 1) * cols, cols)],
            send_sem=ag_send.at[i], recv_sem=ag_recv.at[i], device_id=(q, d), device_id_type=MESH)
        k.start()
        ag.append(k)
    for k in zc:
        k.wait()

    def exchange(v, i):
        return pltpu.make_async_remote_copy(
            src_ref=csend_ref.at[i, v], dst_ref=crecv_ref.at[i, v],
            send_sem=ex_send.at[i, v], recv_sem=ex_recv.at[i, v],
            device_id=(p, sib), device_id_type=MESH)

    def send_sum(v, i, total):
        csend_ref[i, v] = jnp.broadcast_to(jnp.sum(total, axis=0, keepdims=True), total.shape)
        exchange(v, i).start()

    def recv_weight(v, i):
        exchange(v, i).wait()
        return 1.0 / (csend_ref[i, v] + crecv_ref[i, v])

    TA = 512
    for j in range(4):
        if j:
            ag[j - 1].wait_recv()
        lanes = pl.ds(j * cols, cols)
        for v in range(2):
            def score_tile(t, acc, v=v, j=j, lanes=lanes):
                rs = pl.ds(pl.multiple_of(t * TA, TA), TA)
                s = lax.dot_general(z_ref[v, rs, :], c_ref[lanes, :], (((1,), (1,)), ((), ())),
                                    preferred_element_type=F32)
                x = s * (LOG2E / TEMP_TAU)
                f = jnp.exp2(x)
                e = f * f
                f_ref[v, rs, lanes] = f
                e_ref[v, rs, lanes] = e
                if j == 0:
                    x_ref[v, rs, :] = x
                half = f[:, :128] + f[:, 128:]
                if j == 0:
                    d_ref[v, rs, :] = half
                else:
                    d_ref[v, rs, :] += half
                return acc + jnp.sum(groups(e), axis=0)
            acc = lax.fori_loop(0, rows // TA, score_tile, jnp.zeros((8, cols), F32))
            csum_ref[v, :, lanes] = acc
            if j == 3:
                send_sum(v, 0, csum_ref[v])

    TB = 128

    def row_sums(v, t, w, store):
        rs = pl.ds(pl.multiple_of(t * TB, TB), TB)
        ew = groups(e_ref[v, rs, :]) * w[None]
        if store:
            e_ref[v, rs, :] = ew.reshape(TB, allc)
        r = jnp.sum(ew, axis=2, keepdims=True)
        return jnp.broadcast_to(r, (TB // 8, 8, 128))

    def col_sums(v, t, r, acc):
        rs = pl.ds(pl.multiple_of(t * TB, TB), TB)
        q = 1.0 / r
        e = e_ref[v, rs, :].reshape(TB // 8, 8, allc // 128, 128)
        eq = [jnp.sum(e[:, :, k, :] * q, axis=0) for k in range(allc // 128)]
        return acc + jnp.concatenate(eq, axis=1)

    nb = rows // TB
    for i in range(2):
        for v in range(2):
            w = recv_weight(v, i)

            def body(t, carry, v=v, w=w):
                r, acc = carry
                r_new = row_sums(v, t, w, False)
                acc = col_sums(v, t - 1, r, acc)
                return r_new, acc
            carry = (row_sums(v, 0, w, False), jnp.zeros((8, allc), F32))
            r, acc = lax.fori_loop(1, nb, body, carry)
            acc = col_sums(v, nb - 1, r, acc)
            send_sum(v, i + 1, acc)

    for v in range(2):
        w = recv_weight(v, 2)

        def last(t, _, v=v, w=w):
            rs = pl.ds(pl.multiple_of(t * TB, TB), TB)
            r = row_sums(v, t, w, True).reshape(TB, 128)
            dn = jnp.broadcast_to(jnp.sum(d_ref[v, rs, :], axis=1, keepdims=True), (TB, 128))
            r_ref[v, rs, :] = r
            d_ref[v, rs, :] = dn
            return 0
        lax.fori_loop(0, nb, last, 0)

    TC = 128

    def lanes2(a):
        return jnp.concatenate([a, a], axis=1)

    def own(t, acc):
        rs = pl.ds(pl.multiple_of(t * TC, TC), TC)
        qv, pv, lv = [], [], []
        for v in range(2):
            qv.append(1.0 / r_ref[v, rs, :])
            dn = d_ref[v, rs, :]
            pv.append(grad_scale / dn)
            lv.append(jnp.log(dn) * LOG2E)
            s_ref[v, rs, :] = qv[v] * grad_scale
            d_ref[v, rs, :] = pv[v]
        for v, out in ((0, q1_out), (1, q2_out)):
            o = 1 - v
            code = e_ref[v, rs, pl.ds(0, cols)] * lanes2(qv[v])
            out[rs, :] = code
            acc = acc + jnp.sum(groups((x_ref[o, rs, :] - lanes2(lv[o])) * code), axis=0)
            h_ref[o, rs, pl.ds(0, cols)] = (
                f_ref[o, rs, pl.ds(0, cols)] * lanes2(pv[o]) - code * grad_scale).astype(BF16)
        return acc
    lacc = lax.fori_loop(0, rows // TC, own, jnp.zeros((8, cols), F32))
    me = p * 2 + d
    lbuf_ref[me] = lacc[:, :128] + lacc[:, 128:]
    lcs = []
    for i, (q, e) in enumerate(peers):
        k = pltpu.make_async_remote_copy(
            src_ref=lbuf_ref.at[me], dst_ref=lbuf_ref.at[me],
            send_sem=ls_send.at[i], recv_sem=ls_recv.at[i],
            device_id=(q, e), device_id_type=MESH)
        k.start()
        lcs.append(k)
    tdims = (((0,), (0,)), ((), ()))
    gsend_ref[...] = (
        lax.dot_general(h_ref[0, :, pl.ds(0, cols)], z_ref[0], tdims, preferred_element_type=F32)
        + lax.dot_general(h_ref[1, :, pl.ds(0, cols)], z_ref[1], tdims, preferred_element_type=F32))
    gcopy = pltpu.make_async_remote_copy(
        src_ref=gsend_ref, dst_ref=grecv_ref, send_sem=gp_send, recv_sem=gp_recv,
        device_id=(p, sib), device_id_type=MESH)
    gcopy.start()

    TD = 256

    def rest(t, _):
        rs = pl.ds(pl.multiple_of(t * TD, TD), TD)
        for v, out in ((0, g1_out), (1, g2_out)):
            o = 1 - v
            pv = d_ref[v, rs, :]
            sv = s_ref[o, rs, :]
            hs = [h_ref[v, rs, pl.ds(0, cols)]]
            for j in range(1, 4):
                lanes = pl.ds(j * cols, cols)
                hs.append((f_ref[v, rs, lanes] * lanes2(pv) - e_ref[o, rs, lanes] * lanes2(sv)).astype(BF16))
            h = jnp.concatenate(hs, axis=1)
            out[rs, :] = jnp.dot(h, c_ref[...], preferred_element_type=F32)
        return 0
    lax.fori_loop(0, rows // TD, rest, 0)

    for k in lcs:
        k.wait()
    total = lbuf_ref[0]
    for i in range(1, 8):
        total = total + lbuf_ref[i]
    loss_out[0, 0] = jnp.sum(total) * (-LN2 / (2.0 * n_rows_total))
    gcopy.wait()
    gp_out[...] = gsend_ref[...] + grecv_ref[...]
    for k in ag:
        k.wait_send()


def solution(mesh):
    data_size = mesh.shape['data']

    def local_step(emb_one, emb_two, protos):
        rows, dim = emb_one.shape
        cols = protos.shape[0]
        allc = 4 * cols
        V = pltpu.VMEM
        out_shape = (
            V((rows, cols), F32), V((rows, cols), F32),
            jax.ShapeDtypeStruct((1, 1), F32),
            V((rows, dim), F32), V((rows, dim), F32),
            V((cols, dim), F32))
        vspec = pl.BlockSpec(memory_space=pltpu.VMEM)
        DMA = pltpu.SemaphoreType.DMA
        q1, q2, loss, g1, g2, gp = pl.pallas_call(
            functools.partial(kernel, rows * data_size),
            out_shape=out_shape,
            in_specs=[pl.BlockSpec(memory_space=pl.ANY)] * 3,
            out_specs=(vspec, vspec, pl.BlockSpec(memory_space=pltpu.SMEM), vspec, vspec, vspec),
            scratch_shapes=[
                V((2, rows, dim), BF16),
                V((allc, dim), BF16),
                V((2, rows, allc), F32),
                V((2, rows, allc), F32),
                V((2, rows, cols), F32),
                V((2, rows, cols), BF16),
                V((2, rows, 128), F32),
                V((2, rows, 128), F32),
                V((2, rows, 128), F32),
                V((8, 128), F32),
                V((2, 8, allc), F32),
                V((3, 2, 8, allc), F32),
                V((3, 2, 8, allc), F32),
                V((cols, dim), F32),
                V((cols, dim), F32),
                V((8, 8, 128), F32),
                DMA((2,)), DMA(()), DMA((3,)), DMA((3,)), DMA((3, 2)), DMA((3, 2)),
                DMA(()), DMA(()), DMA((7,)), DMA((7,)),
            ],
            compiler_params=pltpu.CompilerParams(collective_id=0, has_side_effects=True,
                                                 vmem_limit_bytes=52 * 1024 * 1024),
        )(emb_one, emb_two, protos)
        return q1, q2, loss.reshape(()), g1, g2, gp

    return jax.shard_map(
        local_step, mesh=mesh,
        in_specs=(P('data', None), P('data', None), P('proto', None)),
        out_specs=(P('data', 'proto'), P('data', 'proto'), P(), P('data', None), P('data', None), P('proto', None)),
        check_vma=False)
```

```python
import functools

import jax
import jax.numpy as jnp
from jax import lax
from jax.experimental import pallas as pl
from jax.experimental.pallas import tpu as pltpu
from jax.sharding import PartitionSpec as P

EPSILON = 0.05
TEMP_TAU = 0.1
LOG2E = 1.4426950408889634
LN2 = 0.6931471805599453
MESH = pl.DeviceIdType.MESH
F32 = jnp.float32
BF16 = jnp.bfloat16


def groups(x):
    return x.reshape(x.shape[0] // 8, 8, x.shape[1])


def kernel(n_rows_total, z1_hbm, z2_hbm, c_hbm,
           q1_out, q2_out, loss_out, g1_out, g2_out, gp_out,
           z_ref, c_ref, e_ref, f_ref, x_ref, h_ref, d_ref, r_ref,
           csum_ref, csend_ref, crecv_ref, gsend_ref, grecv_ref, lbuf_ref,
           zsem, csem, ag_send, ag_recv, ex_send, ex_recv, gp_send, gp_recv, ls_send, ls_recv):
    rows = z1_hbm.shape[0]
    cols = c_hbm.shape[0]
    allc = 4 * cols
    p = lax.axis_index("proto")
    d = lax.axis_index("data")
    px = p + 1 - 2 * lax.rem(p, 2)
    py = lax.rem(p + 2, 4)
    pd = 3 - p
    sib = 1 - d
    grad_scale = 1.0 / (2.0 * n_rows_total * TEMP_TAU)

    barrier = pltpu.get_barrier_semaphore()
    peers = [(p, sib)] + [(q, e) for q in (px, py, pd) for e in (d, sib)]
    for q, e in peers:
        pl.semaphore_signal(barrier, inc=1, device_id=(q, e), device_id_type=MESH)
    cc = pltpu.make_async_copy(c_hbm, c_ref.at[pl.ds(0, cols)], csem)
    cc.start()
    zc = [pltpu.make_async_copy(z, z_ref.at[v], zsem.at[v]) for v, z in enumerate((z1_hbm, z2_hbm))]
    for k in zc:
        k.start()
    cc.wait()
    pl.semaphore_wait(barrier, 7)
    ag = []
    for i, q in enumerate((px, py, pd)):
        k = pltpu.make_async_remote_copy(
            src_ref=c_ref.at[pl.ds(0, cols)], dst_ref=c_ref.at[pl.ds((i + 1) * cols, cols)],
            send_sem=ag_send.at[i], recv_sem=ag_recv.at[i], device_id=(q, d), device_id_type=MESH)
        k.start()
        ag.append(k)
    for k in zc:
        k.wait()

    def exchange(v, i):
        return pltpu.make_async_remote_copy(
            src_ref=csend_ref.at[i, v], dst_ref=crecv_ref.at[i, v],
            send_sem=ex_send.at[i, v], recv_sem=ex_recv.at[i, v],
            device_id=(p, sib), device_id_type=MESH)

    def send_sum(v, i, total):
        csend_ref[i, v] = jnp.broadcast_to(jnp.sum(total, axis=0, keepdims=True), total.shape)
        exchange(v, i).start()

    def recv_weight(v, i):
        exchange(v, i).wait()
        return 1.0 / (csend_ref[i, v] + crecv_ref[i, v])

    TA = 2048
    for j in range(4):
        if j:
            ag[j - 1].wait_recv()
        lanes = pl.ds(j * cols, cols)
        for v in range(2):
            def score_tile(t, acc, v=v, j=j, lanes=lanes):
                rs = pl.ds(pl.multiple_of(t * TA, TA), TA)
                s = lax.dot_general(z_ref[v, rs, :], c_ref[lanes, :], (((1,), (1,)), ((), ())),
                                    preferred_element_type=F32)
                x = s * (LOG2E / TEMP_TAU)
                f = jnp.exp2(x)
                e = f * f
                f_ref[v, rs, lanes] = f
                e_ref[v, rs, lanes] = e
                if j == 0:
                    x_ref[v, rs, :] = x
                return acc + jnp.sum(groups(e), axis=0)
            acc = lax.fori_loop(0, rows // TA, score_tile, jnp.zeros((8, cols), F32))
            csum_ref[v, :, lanes] = acc
            if j == 3:
                send_sum(v, 0, csum_ref[v])

    TB = 256
    nb = rows // TB
    nk = allc // 128

    def tile(t, n):
        return pl.ds(pl.multiple_of(t * n, n), n)

    def row_sums(v, t, w):
        rs = tile(t, TB)
        part = groups(e_ref[v, rs, pl.ds(0, 128)]) * w[0][None]
        for k in range(1, nk):
            part = part + groups(e_ref[v, rs, pl.ds(k * 128, 128)]) * w[k][None]
        r = jnp.broadcast_to(jnp.sum(part, axis=2, keepdims=True), part.shape)
        r_ref[v, rs, :] = r.reshape(TB, 128)

    def col_sums(v, t, acc):
        rs = tile(t, TB)
        q = 1.0 / groups(r_ref[v, rs, :])
        return tuple(acc[k] + jnp.sum(groups(e_ref[v, rs, pl.ds(k * 128, 128)]) * q, axis=0)
                     for k in range(nk))

    def split(w):
        return tuple(w[:, k * 128:(k + 1) * 128] for k in range(nk))

    for i in range(2):
        for v in range(2):
            w = split(recv_weight(v, i))

            def body(t, acc, v=v, w=w):
                acc = col_sums(v, t - 1, acc)
                row_sums(v, t, w)
                return acc
            row_sums(v, 0, w)
            acc = lax.fori_loop(1, nb, body, (jnp.zeros((8, 128), F32),) * nk)
            acc = col_sums(v, nb - 1, acc)
            send_sum(v, i + 1, jnp.concatenate(acc, axis=1))

    for v in range(2):
        wfull = recv_weight(v, 2)
        csum_ref[v] = wfull
        w = split(wfull)

        def last(t, _, v=v, w=w):
            rs = tile(t, TB)
            dsum = f_ref[v, rs, pl.ds(0, 128)]
            for k in range(1, nk):
                dsum = dsum + f_ref[v, rs, pl.ds(k * 128, 128)]
            row_sums(v, t, w)
            d_ref[v, rs, :] = jnp.broadcast_to(jnp.sum(dsum, axis=1, keepdims=True), (TB, 128))
            return 0
        lax.fori_loop(0, nb, last, 0)

    TC = 128

    def lanes2(a):
        return jnp.concatenate([a, a], axis=1)

    def scaled(v, rs, lanes):
        n = rs.size
        return (groups(e_ref[v, rs, lanes]) * csum_ref[v, :, lanes][None]).reshape(n, lanes.size)

    def own(t, acc):
        rs = tile(t, TC)
        qv, pv, lv = [], [], []
        for v in range(2):
            qv.append(1.0 / r_ref[v, rs, :])
            dn = d_ref[v, rs, :]
            pv.append(grad_scale / dn)
            lv.append(jnp.log2(dn))
            r_ref[v, rs, :] = qv[v] * grad_scale
            d_ref[v, rs, :] = pv[v]
        for v, out in ((0, q1_out), (1, q2_out)):
            o = 1 - v
            code = scaled(v, rs, pl.ds(0, cols)) * lanes2(qv[v])
            out[rs, :] = code
            acc = acc + jnp.sum(groups((x_ref[o, rs, :] - lanes2(lv[o])) * code), axis=0)
            h_ref[o, rs, pl.ds(0, cols)] = (
                f_ref[o, rs, pl.ds(0, cols)] * lanes2(pv[o]) - code * grad_scale).astype(BF16)
        return acc
    lacc = lax.fori_loop(0, rows // TC, own, jnp.zeros((8, cols), F32))
    me = p * 2 + d
    lbuf_ref[me] = lacc[:, :128] + lacc[:, 128:]
    lcs = []
    for i, (q, e) in enumerate(peers):
        k = pltpu.make_async_remote_copy(
            src_ref=lbuf_ref.at[me], dst_ref=lbuf_ref.at[me],
            send_sem=ls_send.at[i], recv_sem=ls_recv.at[i],
            device_id=(q, e), device_id_type=MESH)
        k.start()
        lcs.append(k)
    tdims = (((0,), (0,)), ((), ()))
    gsend_ref[...] = (
        lax.dot_general(h_ref[0, :, pl.ds(0, cols)], z_ref[0], tdims, preferred_element_type=F32)
        + lax.dot_general(h_ref[1, :, pl.ds(0, cols)], z_ref[1], tdims, preferred_element_type=F32))
    gcopy = pltpu.make_async_remote_copy(
        src_ref=gsend_ref, dst_ref=grecv_ref, send_sem=gp_send, recv_sem=gp_recv,
        device_id=(p, sib), device_id_type=MESH)
    gcopy.start()

    TD = 256

    def rest(t, _):
        rs = tile(t, TD)
        both = []
        for v in range(2):
            o = 1 - v
            pv = d_ref[v, rs, :]
            sv = r_ref[o, rs, :]
            hs = [h_ref[v, rs, pl.ds(0, cols)]]
            for j in range(1, 4):
                lanes = pl.ds(j * cols, cols)
                hs.append((f_ref[v, rs, lanes] * lanes2(pv) - scaled(o, rs, lanes) * lanes2(sv)).astype(BF16))
            both.append(jnp.concatenate(hs, axis=1))
        g = jnp.dot(jnp.concatenate(both, axis=0), c_ref[...], preferred_element_type=F32)
        g1_out[rs, :] = g[:TD]
        g2_out[rs, :] = g[TD:]
        return 0
    lax.fori_loop(0, rows // TD, rest, 0)

    for k in lcs:
        k.wait()
    total = lbuf_ref[0]
    for i in range(1, 8):
        total = total + lbuf_ref[i]
    loss_out[0, 0] = jnp.sum(total) * (-LN2 / (2.0 * n_rows_total))
    gcopy.wait()
    gp_out[...] = gsend_ref[...] + grecv_ref[...]
    for k in ag:
        k.wait_send()


def solution(mesh):
    data_size = mesh.shape['data']

    def local_step(emb_one, emb_two, protos):
        rows, dim = emb_one.shape
        cols = protos.shape[0]
        allc = 4 * cols
        V = pltpu.VMEM
        out_shape = (
            V((rows, cols), F32), V((rows, cols), F32),
            jax.ShapeDtypeStruct((1, 1), F32),
            V((rows, dim), F32), V((rows, dim), F32),
            V((cols, dim), F32))
        vspec = pl.BlockSpec(memory_space=pltpu.VMEM)
        DMA = pltpu.SemaphoreType.DMA
        q1, q2, loss, g1, g2, gp = pl.pallas_call(
            functools.partial(kernel, rows * data_size),
            out_shape=out_shape,
            in_specs=[pl.BlockSpec(memory_space=pl.ANY)] * 3,
            out_specs=(vspec, vspec, pl.BlockSpec(memory_space=pltpu.SMEM), vspec, vspec, vspec),
            scratch_shapes=[
                V((2, rows, dim), BF16),
                V((allc, dim), BF16),
                V((2, rows, allc), F32),
                V((2, rows, allc), F32),
                V((2, rows, cols), F32),
                V((2, rows, cols), BF16),
                V((2, rows, 128), F32),
                V((2, rows, 128), F32),
                V((2, 8, allc), F32),
                V((3, 2, 8, allc), F32),
                V((3, 2, 8, allc), F32),
                V((cols, dim), F32),
                V((cols, dim), F32),
                V((8, 8, 128), F32),
                DMA((2,)), DMA(()), DMA((3,)), DMA((3,)), DMA((3, 2)), DMA((3, 2)),
                DMA(()), DMA(()), DMA((7,)), DMA((7,)),
            ],
            compiler_params=pltpu.CompilerParams(collective_id=0, has_side_effects=True,
                                                 vmem_limit_bytes=52 * 1024 * 1024),
        )(emb_one, emb_two, protos)
        return q1, q2, loss.reshape(()), g1, g2, gp

    return jax.shard_map(
        local_step, mesh=mesh,
        in_specs=(P('data', None), P('data', None), P('proto', None)),
        out_specs=(P('data', 'proto'), P('data', 'proto'), P(), P('data', None), P('data', None), P('proto', None)),
        check_vma=False)
```
